32 devices in a mesh: slab: 16 (over z, y, x), energy: 2 (over core).
Axes of the slice: x: 2, y: 2, z: 4, core: 2. Of those that a mesh axis runs over, the one named last changes fastest.
Arguments:
- onsite_energy: float32 [32, 128], P('slab'), may hold values from -0.3 to 0.3
- onsite_mixing: float32 [32, 128, 128], P('slab'), may hold values from -0.15625 to 0.15625
- hop_strength: float32 [32, 128], P('slab'), may hold values from 0.8 to 1.2
- hop_mixing: float32 [32, 128, 128], P('slab'), may hold values from -0.15625 to 0.15625
- energy: float32 [2], P('energy'), parts along dimension 0, may hold values from -0.4 to 0.4
- broadening: float32 [2], P('energy'), parts along dimension 0, may hold values from 0.01 to 0.025
Outputs:
- green_real: float32 [64, 128, 128], P(('energy', 'slab')), parts along dimension 0
- green_imag: float32 [64, 128, 128], P(('energy', 'slab')), parts along dimension 0
The draws below stay inside these ranges and needn't reach their ends.
There are 2 independent parts, one for each index of `energy`. The reference program is written for one: setup_inputs(seed, part) draws one part's arguments, and reference() takes and returns one part's arrays. A program takes and returns all parts, laid end to end along the dimension named above; an argument that names none is the same for every part. Nothing has to cross between parts.
All inputs are finite; a program needn't handle non-finite values.
Results may differ from the reference program's by a relative error of at most 0.0007.
Values sent between devices are 32-bit elements; how exact they have to be, the bound alone decides.
A program may use at most 128 MiB of HBM per device.

```python
import math
import jax
import jax.numpy as jnp
from jax import lax

ORB = 128
SLABS = 32


def steps_of(own_key, extent, cuts, smallest, largest):
    loudness = 1.0
    for position, shards_of in cuts:
        heights = jax.random.uniform(jax.random.fold_in(jax.random.fold_in(own_key, 6), position), (shards_of,), jnp.float32, smallest / len(cuts), largest / len(cuts))
        loudness = loudness * jnp.repeat(jnp.exp(heights), extent[position] // shards_of).reshape((-1,) + (1,) * (len(extent) - 1 - position))
    return loudness


def centred(rng, shape, scale, bound, pieces=(), kind=jnp.bfloat16):
    drawn = jax.random.normal(rng, shape, jnp.float32) * scale
    if len(pieces) > 0:
        drawn = steps_of(rng, shape, pieces, -0.22, 0.18) * drawn
    return jnp.clip(drawn, min=-bound, max=bound).astype(kind)


def setup_inputs(seed: int = 0, part: int = 0) -> dict:
    seeds = jax.random.split(jax.random.key(seed), 7)
    own_keys = jax.random.split(jax.random.fold_in(seeds[6], part), 7)
    onsite_energy = jnp.clip(jax.random.uniform(seeds[0], (SLABS, ORB), jnp.float32, -0.3, 0.3) * steps_of(seeds[0], (SLABS, ORB), ((0, 16),), -0.4, 0.0), -0.3, 0.3)
    onsite_mixing = centred(seeds[1], (SLABS, ORB, ORB), (10 * ORB) ** -0.5, 0.15625, ((0, 16),), jnp.float32)
    hop_strength = jnp.clip(0.8 + 0.40000004 * jax.random.uniform(seeds[2], (SLABS, ORB), jnp.float32) ** steps_of(seeds[2], (SLABS, ORB), ((0, 16),), -0.2, 0.2), 0.8, 1.2)
    hop_mixing = centred(seeds[3], (SLABS, ORB, ORB), (10 * ORB) ** -0.5, 0.15625, ((0, 16),), jnp.float32)
    energy = jnp.clip(jax.random.uniform(own_keys[4], (1,), jnp.float32, -0.4, 0.4), -0.4, 0.4)
    broadening = jnp.clip(jnp.exp(jax.random.uniform(own_keys[5], (1,), jnp.float32, math.log(0.01), math.log(0.025))), 0.01, 0.025)
    return dict(onsite_energy=onsite_energy, onsite_mixing=onsite_mixing, hop_strength=hop_strength, hop_mixing=hop_mixing, energy=energy, broadening=broadening)


def real_product(first, second):
    return jnp.dot(first.astype(jnp.float32), second.astype(jnp.float32), precision=lax.Precision.HIGHEST, preferred_element_type=jnp.float32)

def complex_product(first, second):
    return (real_product(first[0], second[0]) - real_product(first[1], second[1]), real_product(first[0], second[1]) + real_product(first[1], second[0]))

def invert_exact(real_part, imag_part):
    orbitals = real_part.shape[0]
    stacked = jnp.concatenate([jnp.concatenate([real_part, -imag_part], axis=1), jnp.concatenate([imag_part, real_part], axis=1)], axis=0)
    whole = jnp.linalg.inv(stacked)
    return (whole[:orbitals, :orbitals], whole[orbitals:, :orbitals])

def reference(onsite_energy, onsite_mixing, hop_strength, hop_mixing, energy, broadening):
    orbitals = onsite_mixing.shape[1]
    identity = jnp.eye(orbitals, dtype=jnp.float32)
    hamilton = jax.vmap(jnp.diag)(onsite_energy) + 0.5 * (onsite_mixing + jnp.swapaxes(onsite_mixing, 1, 2))
    diagonal_real = energy[0] * identity - hamilton
    diagonal_imag = broadening[0] * identity
    couplings = jax.vmap(jnp.diag)(hop_strength) + hop_mixing
    empty_block = jnp.zeros((orbitals, orbitals), jnp.float32)

    def sweep_forward(carried, inputs):
        previous_real, previous_imag, coupling = carried
        block_real, next_coupling = inputs
        reduced_real = block_real - real_product(real_product(coupling.T, previous_real), coupling)
        reduced_imag = diagonal_imag - real_product(real_product(coupling.T, previous_imag), coupling)
        connected = invert_exact(reduced_real, reduced_imag)
        return ((connected[0], connected[1], next_coupling), connected)
    ending, connected = lax.scan(sweep_forward, (empty_block, empty_block, empty_block), (diagonal_real, couplings))

    def sweep_backward(following, inputs):
        here_real, here_imag, coupling = inputs
        left_side = (real_product(here_real, coupling), real_product(here_imag, coupling))
        middle = complex_product(left_side, following)
        right_side = (real_product(middle[0], coupling.T), real_product(middle[1], coupling.T))
        correction = complex_product(right_side, (here_real, here_imag))
        result = (here_real + correction[0], here_imag + correction[1])
        return (result, result)
    final_block = (connected[0][-1], connected[1][-1])
    leftover, earlier = lax.scan(sweep_backward, final_block, (connected[0][:-1], connected[1][:-1], couplings[:-1]), reverse=True)
    green_real = jnp.concatenate([earlier[0], final_block[0][None]], axis=0)
    green_imag = jnp.concatenate([earlier[1], final_block[1][None]], axis=0)
    return (green_real, green_imag)
```

```python
import functools

import jax
import jax.numpy as jnp
from jax import lax
from jax.experimental import pallas as pl
from jax.experimental.pallas import tpu as pltpu
from jax.sharding import PartitionSpec as P

REFINEMENTS = 1
TILE = 8


def dot(first, second):
    return jnp.dot(
        first, second, precision=lax.Precision.HIGHEST, preferred_element_type=jnp.float32
    )


def product(first, second):
    columns = second[0].shape[1]
    left = jnp.concatenate([first[0], first[1]], axis=1)
    right = jnp.concatenate(
        [
            jnp.concatenate([second[0], second[1]], axis=1),
            jnp.concatenate([-second[1], second[0]], axis=1),
        ],
        axis=0,
    )
    out = dot(left, right)
    return (out[:, :columns], out[:, columns:])


def flipped(block):
    return (block[0].T, block[1].T)


def rows(*blocks):
    return tuple(jnp.concatenate([b[part] for b in blocks], axis=0) for part in (0, 1))


def cols(*blocks):
    return tuple(jnp.concatenate([b[part] for b in blocks], axis=1) for part in (0, 1))


def chosen(flag, first, second):
    return tuple(jnp.where(flag, a, b) for a, b in zip(first, second))


def read(ref, index=0):
    return (ref[index], ref[index + 1])


def write(ref, block, index=0):
    ref[index] = block[0]
    ref[index + 1] = block[1]


def eye(size):
    row = lax.broadcasted_iota(jnp.int32, (size, size), 0)
    column = lax.broadcasted_iota(jnp.int32, (size, size), 1)
    return row == column


def inverse(block):
    size = block[0].shape[0]
    lane = lax.broadcasted_iota(jnp.int32, (1, size), 1)
    sub = lax.broadcasted_iota(jnp.int32, (TILE, size), 0)

    def trip(_, carried):
        real, imag = carried
        for j in range(TILE):
            pivot_r, pivot_i = real[j : j + 1, j : j + 1], imag[j : j + 1, j : j + 1]
            scale = 1.0 / (pivot_r * pivot_r + pivot_i * pivot_i)
            q_r, q_i = pivot_r * scale, -pivot_i * scale
            row_r, row_i = real[j : j + 1, :], imag[j : j + 1, :]
            here = lane == j
            new_r = jnp.where(here, q_r, row_r * q_r - row_i * q_i)
            new_i = jnp.where(here, q_i, row_r * q_i + row_i * q_r)
            use_r = jnp.where(here, 1.0 + q_r, new_r)
            col_r, col_i = real[:, j : j + 1], imag[:, j : j + 1]
            real, imag = (
                real - (col_r * use_r - col_i * new_i),
                imag - (col_r * new_i + col_i * use_r),
            )
            at = sub == j
            real = jnp.concatenate([jnp.where(at, new_r, real[:TILE]), real[TILE:]], axis=0)
            imag = jnp.concatenate([jnp.where(at, new_i, imag[:TILE]), imag[TILE:]], axis=0)
        real = jnp.concatenate([real[TILE:], real[:TILE]], axis=0)
        imag = jnp.concatenate([imag[TILE:], imag[:TILE]], axis=0)
        return pltpu.roll(real, size - TILE, 1), pltpu.roll(imag, size - TILE, 1)

    estimate = lax.fori_loop(0, size // TILE, trip, block)
    for _ in range(REFINEMENTS):
        residue = product(block, estimate)
        one = jnp.where(eye(size), 1.0, 0.0)
        fix = product(estimate, (one - residue[0], -residue[1]))
        estimate = (estimate[0] + fix[0], estimate[1] + fix[1])
    return estimate


def begin(energy_ref, broad_ref, flags_ref, onsite_ref, mix_ref, hop_ref, hopmix_ref,
          crit_ref, rest_ref, own_ref):
    size = mix_ref.shape[1]
    unit = eye(size)
    diagonal_i = jnp.where(unit, broad_ref[0], 0.0)

    def onsite(k):
        mixing = mix_ref[k]
        diagonal = jnp.where(unit, energy_ref[0] - onsite_ref[k : k + 1, :], 0.0)
        return diagonal - 0.5 * (mixing + mixing.T)

    def coupling(k):
        return jnp.where(unit, hop_ref[k : k + 1, :], 0.0) + hopmix_ref[k]

    lower = coupling(0)
    upper = jnp.where(flags_ref[0] > 0, 0.0, coupling(1))
    middle = inverse((onsite(1), diagonal_i))
    legs = jnp.concatenate([lower.T, upper], axis=1)
    weighted = dot(jnp.concatenate([middle[0], middle[1]], axis=0), legs)
    to_low = (weighted[:size, :size], weighted[size:, :size])
    to_high = (weighted[:size, size:], weighted[size:, size:])
    both = jnp.concatenate(
        [to_low[0], to_low[1], to_high[0], to_high[1]], axis=1
    )
    outs = dot(jnp.concatenate([lower, upper.T], axis=0), both)
    alpha = (onsite(0) - outs[:size, :size], diagonal_i - outs[:size, size : 2 * size])
    link = (outs[:size, 2 * size : 3 * size], outs[:size, 3 * size :])
    beta = (outs[size:, 2 * size : 3 * size], outs[size:, 3 * size :])
    is_high = flags_ref[1] > 0
    write(crit_ref, chosen(is_high, alpha, beta))
    write(rest_ref, link)
    write(rest_ref, chosen(is_high, beta, alpha), 2)
    write(own_ref, middle)
    write(own_ref, to_low, 2)
    write(own_ref, to_high, 4)


def eliminate(flags_ref, mine_ref, other_ref, y_ref):
    mine, other = read(mine_ref), read(other_ref)
    sign = jnp.where(flags_ref[0] > 0, 1.0, -1.0)
    write(y_ref, inverse((sign * (mine[0] - other[0]), sign * (mine[1] - other[1]))))


def merge(flags_ref, y_ref, mine_ref, other_ref, crit_ref, rest_ref):
    size = y_ref.shape[1]
    high = flags_ref[0] > 0
    next_high = flags_ref[1] > 0
    mine_link, other_link = read(mine_ref), read(other_ref)
    mine_rest, other_rest = read(mine_ref, 2), read(other_ref, 2)
    low_link = chosen(high, other_link, mine_link)
    high_link = chosen(high, mine_link, other_link)
    alpha = chosen(high, other_rest, mine_rest)
    beta = chosen(high, mine_rest, other_rest)
    weighted = product(rows(low_link, flipped(high_link)), read(y_ref))
    outs = product(weighted, cols(flipped(low_link), high_link))
    alpha = tuple(a - o[:size, :size] for a, o in zip(alpha, outs))
    link = tuple(o[:size, size:] for o in outs)
    beta = tuple(b + o[size:, size:] for b, o in zip(beta, outs))
    write(crit_ref, chosen(next_high, alpha, beta))
    write(rest_ref, link)
    write(rest_ref, chosen(next_high, beta, alpha), 2)


def follow(flags_ref, y_ref, mine_ref, other_ref, first_ref, second_ref, first_out, second_out):
    size = y_ref.shape[1]
    high = flags_ref[0] > 0
    mine_link, other_link = read(mine_ref), read(other_ref)
    low_link = chosen(high, other_link, mine_link)
    high_link = chosen(high, mine_link, other_link)
    states = [[read(ref, 2 * k) for k in range(3)] for ref in (first_ref, second_ref)]
    used = [chosen(high, state[1], state[2]) for state in states]
    weighted = product(rows(*used), read(y_ref))
    legs = product(weighted, cols(flipped(low_link), high_link))
    zero = jnp.zeros((size, size), jnp.float32)
    for k, (state, out) in enumerate(zip(states, (first_out, second_out))):
        part = slice(k * size, (k + 1) * size)
        own = product((weighted[0][part], weighted[1][part]), flipped(used[k]))
        write(out, (state[0][0] + own[0], state[0][1] + own[1]))
        down = tuple(
            jnp.where(high, zero, s) + leg[part, :size] for s, leg in zip(state[1], legs)
        )
        up = tuple(
            jnp.where(high, s, zero) + leg[part, size:] for s, leg in zip(state[2], legs)
        )
        write(out, down, 2)
        write(out, up, 4)


def finish(alpha_ref, first_ref, second_ref, real_ref, imag_ref):
    size = alpha_ref.shape[1]
    top = inverse(read(alpha_ref))
    states = [[read(ref, 2 * k) for k in range(2)] for ref in (first_ref, second_ref)]
    weighted = product(rows(states[0][1], states[1][1]), top)
    for k, state in enumerate(states):
        part = slice(k * size, (k + 1) * size)
        own = product((weighted[0][part], weighted[1][part]), flipped(state[1]))
        real_ref[k] = state[0][0] + own[0]
        imag_ref[k] = state[0][1] + own[1]


VMEM = pl.BlockSpec(memory_space=pltpu.VMEM)
SMEM = pl.BlockSpec(memory_space=pltpu.SMEM)


def launch(body, scalars, arrays, shapes, flops):
    cost = pl.CostEstimate(flops=flops, bytes_accessed=1 << 20, transcendentals=0)
    return pl.pallas_call(
        body,
        out_shape=[jax.ShapeDtypeStruct(s, jnp.float32) for s in shapes],
        in_specs=[SMEM] * len(scalars) + [VMEM] * len(arrays),
        out_specs=[VMEM] * len(shapes),
        cost_estimate=cost,
        name=body.__name__,
    )(*scalars, *arrays)


INVERSE_FLOPS = 5 * 10**9
SMALL_FLOPS = 10**9


def shards(onsite_energy, onsite_mixing, hop_strength, hop_mixing, energy, broadening):
    size = onsite_mixing.shape[1]
    count = lax.axis_size("slab")
    levels = count.bit_length() - 1
    position = lax.axis_index("slab")

    def bit(level):
        if level >= levels:
            return jnp.int32(1)
        return ((position >> level) & 1).astype(jnp.int32)

    is_last = (position == count - 1).astype(jnp.int32)
    crit, rest, second = launch(
        begin,
        (energy, broadening, jnp.stack([is_last, bit(0)])),
        (onsite_energy, onsite_mixing, hop_strength, hop_mixing),
        ((2, size, size), (4, size, size), (6, size, size)),
        INVERSE_FLOPS,
    )
    one = jnp.eye(size, dtype=jnp.float32)
    zero = jnp.zeros((size, size), jnp.float32)
    first = jnp.stack([zero, zero, one, zero, zero, zero])
    for level in range(levels):
        flags = jnp.stack([bit(level), bit(level + 1)])
        pairs = [(i, i ^ (1 << level)) for i in range(count)]
        crit_other = lax.ppermute(crit, "slab", pairs)
        if level == levels - 1:
            pairs = [(i, j) for i, j in pairs if i < j]
        rest_other = lax.ppermute(rest, "slab", pairs)
        (y,) = launch(eliminate, (flags,), (crit, crit_other), ((2, size, size),), INVERSE_FLOPS)
        mine = rest
        crit, rest = launch(
            merge, (flags,), (y, mine, rest_other),
            ((2, size, size), (4, size, size)), SMALL_FLOPS,
        )
        first, second = launch(
            follow, (flags,), (y, mine, rest_other, first, second),
            ((6, size, size), (6, size, size)), SMALL_FLOPS,
        )
    real, imag = launch(
        finish, (), (crit, first, second), ((2, size, size), (2, size, size)), INVERSE_FLOPS
    )
    return real, imag


def solution(mesh):
    return jax.shard_map(
        shards,
        mesh=mesh,
        in_specs=(
            P("slab", None),
            P("slab", None, None),
            P("slab", None),
            P("slab", None, None),
            P("energy"),
            P("energy"),
        ),
        out_specs=(P(("energy", "slab"), None, None), P(("energy", "slab"), None, None)),
        check_vma=False,
    )
```

```python
import functools

import jax
import jax.numpy as jnp
from jax import lax
from jax.experimental import pallas as pl
from jax.experimental.pallas import tpu as pltpu
from jax.sharding import PartitionSpec as P

TILE = 8


def dot(first, second, precision=lax.Precision.HIGHEST):
    return jnp.dot(first, second, precision=precision, preferred_element_type=jnp.float32)


def product(first, second, precision=lax.Precision.HIGHEST):
    columns = second[0].shape[1]
    left = jnp.concatenate([first[0], first[1]], axis=1)
    right = jnp.concatenate(
        [
            jnp.concatenate([second[0], second[1]], axis=1),
            jnp.concatenate([-second[1], second[0]], axis=1),
        ],
        axis=0,
    )
    out = dot(left, right, precision)
    return (out[:, :columns], out[:, columns:])


def flipped(block):
    return (block[0].T, block[1].T)


def rows(*blocks):
    return tuple(jnp.concatenate([b[part] for b in blocks], axis=0) for part in (0, 1))


def cols(*blocks):
    return tuple(jnp.concatenate([b[part] for b in blocks], axis=1) for part in (0, 1))


def chosen(flag, first, second):
    return tuple(jnp.where(flag, a, b) for a, b in zip(first, second))


def read(ref, *index):
    return (ref[(*index[:-1], index[-1])], ref[(*index[:-1], index[-1] + 1)])


def write(ref, block, *index):
    ref[(*index[:-1], index[-1])] = block[0]
    ref[(*index[:-1], index[-1] + 1)] = block[1]


def eye(size):
    row = lax.broadcasted_iota(jnp.int32, (size, size), 0)
    column = lax.broadcasted_iota(jnp.int32, (size, size), 1)
    return row == column


def times(first_r, first_i, second_r, second_i):
    return (first_r * second_r - first_i * second_i, first_r * second_i + first_i * second_r)


def reciprocal(value):
    guess = pltpu.reciprocal(value, approx=True)
    guess = guess * (2.0 - value * guess)
    return guess * (2.0 - value * guess)


def inverse(block):
    size = block[0].shape[0]
    lane = lax.broadcasted_iota(jnp.int32, (TILE, size), 1)
    sub = lax.broadcasted_iota(jnp.int32, (TILE, size), 0)
    keep = lax.broadcasted_iota(jnp.int32, (size - TILE, size), 1) >= TILE

    def spread(column):
        return jnp.broadcast_to(column, (TILE, size))

    def trip(_, carried):
        real, imag = carried
        top_r, top_i = real[:TILE], imag[:TILE]
        columns = [
            (spread(top_r[:, j : j + 1]), spread(top_i[:, j : j + 1])) for j in range(TILE)
        ]
        for k in range(TILE):
            col_r, col_i = columns[k]
            pivot_r, pivot_i = col_r[k : k + 1], col_i[k : k + 1]
            scale = reciprocal(pivot_r * pivot_r + pivot_i * pivot_i)
            q_r, q_i = pivot_r * scale, -pivot_i * scale
            at = sub == k
            col_r, col_i = jnp.where(at, -1.0, col_r), jnp.where(at, 0.0, col_i)
            for j in range(k + 1, TILE):
                old_r, old_i = columns[j]
                t_r, t_i = times(old_r[k : k + 1], old_i[k : k + 1], q_r, q_i)
                u_r, u_i = times(col_r, col_i, t_r, t_i)
                columns[j] = (jnp.where(at, 0.0, old_r) - u_r, jnp.where(at, 0.0, old_i) - u_i)
            row_r, row_i = times(top_r[k : k + 1], top_i[k : k + 1], q_r, q_i)
            here = lane[:1] == k
            row_r, row_i = jnp.where(here, q_r, row_r), jnp.where(here, q_i, row_i)
            u_r, u_i = times(col_r, col_i, row_r, row_i)
            gone = at | (lane == k)
            top_r = jnp.where(gone, 0.0, top_r) - u_r
            top_i = jnp.where(gone, 0.0, top_i) - u_i
        old_r, old_i = real[TILE:], imag[TILE:]
        new_r, new_i = jnp.where(keep, old_r, 0.0), jnp.where(keep, old_i, 0.0)
        for k in range(TILE):
            u_r, u_i = times(
                old_r[:, k : k + 1], old_i[:, k : k + 1], top_r[k : k + 1], top_i[k : k + 1]
            )
            new_r, new_i = new_r - u_r, new_i - u_i
        real = jnp.concatenate([new_r, top_r], axis=0)
        imag = jnp.concatenate([new_i, top_i], axis=0)
        return pltpu.roll(real, size - TILE, 1), pltpu.roll(imag, size - TILE, 1)

    estimate = lax.fori_loop(0, size // TILE, trip, block)
    residue = product(block, estimate)
    one = jnp.where(eye(size), 1.0, 0.0)
    fix = product(estimate, (one - residue[0], -residue[1]), lax.Precision.DEFAULT)
    return (estimate[0] + fix[0], estimate[1] + fix[1])


def wire(count, energy_ref, broad_ref, onsite_ref, mix_ref, hop_ref, hopmix_ref, real_ref, imag_ref,
         crit_out, crit_in, rest_out, rest_in, own_ref, crit_sent, crit_got, rest_sent, rest_got):
    levels = count.bit_length() - 1
    size = mix_ref.shape[1]
    me = lax.axis_index("slab")

    def bit(stride):
        return (me // stride) % 2

    def partner(stride):
        return me + stride - 2 * stride * bit(stride)

    def copies(level, stride):
        target = {"slab": partner(stride)}
        return tuple(
            pltpu.make_async_remote_copy(
                src_ref=out.at[level], dst_ref=into.at[level], send_sem=sent.at[level],
                recv_sem=got.at[level], device_id=target,
                device_id_type=pl.DeviceIdType.MESH,
            )
            for out, into, sent, got in (
                (crit_out, crit_in, crit_sent, crit_got),
                (rest_out, rest_in, rest_sent, rest_got),
            )
        )

    barrier = pltpu.get_barrier_semaphore()
    for level in range(levels):
        pl.semaphore_signal(
            barrier, inc=1, device_id={"slab": partner(1 << level)},
            device_id_type=pl.DeviceIdType.MESH,
        )

    unit = eye(size)
    diagonal_i = jnp.where(unit, broad_ref[0], 0.0)

    def onsite(k):
        mixing = mix_ref[k]
        diagonal = jnp.where(unit, energy_ref[0] - onsite_ref[k : k + 1, :], 0.0)
        return diagonal - 0.5 * (mixing + mixing.T)

    def coupling(k):
        return jnp.where(unit, hop_ref[k : k + 1, :], 0.0) + hopmix_ref[k]

    middle = inverse((onsite(1), diagonal_i))
    lower = coupling(0)
    upper = jnp.where(me == count - 1, 0.0, coupling(1))
    weighted = dot(
        jnp.concatenate([middle[0], middle[1]], axis=0),
        jnp.concatenate([lower.T, upper], axis=1),
    )
    to_low = (weighted[:size, :size], weighted[size:, :size])
    to_high = (weighted[:size, size:], weighted[size:, size:])
    outs = dot(
        jnp.concatenate([lower, upper.T], axis=0),
        jnp.concatenate([to_low[0], to_low[1], to_high[0], to_high[1]], axis=1),
    )
    alpha = (onsite(0) - outs[:size, :size], diagonal_i - outs[:size, size : 2 * size])
    link = (outs[:size, 2 * size : 3 * size], outs[:size, 3 * size :])
    beta = (outs[size:, 2 * size : 3 * size], outs[size:, 3 * size :])
    high = bit(1) > 0
    write(crit_out, chosen(high, alpha, beta), 0, 0)
    write(rest_out, link, 0, 0)
    write(rest_out, chosen(high, beta, alpha), 0, 2)
    zero = jnp.zeros((size, size), jnp.float32)
    one = jnp.where(unit, 1.0, 0.0)
    write(own_ref, (zero, zero), 0, 0)
    write(own_ref, (one, zero), 0, 2)
    write(own_ref, (zero, zero), 0, 4)
    write(own_ref, middle, 1, 0)
    write(own_ref, to_low, 1, 2)
    write(own_ref, to_high, 1, 4)
    pl.semaphore_wait(barrier, levels)
    for copy in copies(0, 1):
        copy.start()

    def eliminated(level, high):
        sign = jnp.where(high, 1.0, -1.0)
        mine, other = read(crit_out, level, 0), read(crit_in, level, 0)
        return inverse((sign * (mine[0] - other[0]), sign * (mine[1] - other[1])))

    def links(level, high):
        mine, other = read(rest_out, level, 0), read(rest_in, level, 0)
        return chosen(high, other, mine), chosen(high, mine, other)

    def ends(level, high):
        mine, other = read(rest_out, level, 2), read(rest_in, level, 2)
        return chosen(high, other, mine), chosen(high, mine, other)

    def step(level, stride):
        high = bit(stride) > 0
        crit, rest = copies(level, stride)
        crit.wait_recv()
        y = eliminated(level, high)
        rest.wait_recv()
        low_link, high_link = links(level, high)
        alpha, beta = ends(level, high)
        legs = cols(flipped(low_link), high_link)
        weighted = product(rows(low_link, flipped(high_link)), y)
        outs = product(weighted, legs)
        alpha = tuple(a - o[:size, :size] for a, o in zip(alpha, outs))
        link = tuple(o[:size, size:] for o in outs)
        beta = tuple(b + o[size:, size:] for b, o in zip(beta, outs))
        following = bit(2 * stride) > 0
        write(crit_out, chosen(following, alpha, beta), level + 1, 0)
        write(rest_out, link, level + 1, 0)
        write(rest_out, chosen(following, beta, alpha), level + 1, 2)
        for copy in copies(level + 1, 2 * stride):
            copy.start()
        states = [[read(own_ref, k, 2 * piece) for piece in range(3)] for k in range(2)]
        used = [chosen(high, state[1], state[2]) for state in states]
        weighted = product(rows(*used), y)
        moved = product(weighted, legs)
        for k, state in enumerate(states):
            part = slice(k * size, (k + 1) * size)
            own = product((weighted[0][part], weighted[1][part]), flipped(used[k]))
            write(own_ref, tuple(s + o for s, o in zip(state[0], own)), k, 0)
            down = tuple(
                jnp.where(high, 0.0, s) + m[part, :size] for s, m in zip(state[1], moved)
            )
            up = tuple(
                jnp.where(high, s, 0.0) + m[part, size:] for s, m in zip(state[2], moved)
            )
            write(own_ref, down, k, 2)
            write(own_ref, up, k, 4)
        return 2 * stride

    stride = lax.fori_loop(0, levels - 1, step, jnp.int32(1))
    last = levels - 1
    high = bit(stride) > 0
    crit, rest = copies(last, stride)
    crit.wait_recv()
    y = eliminated(last, high)
    rest.wait_recv()
    low_link, _ = links(last, high)
    alpha, _ = ends(last, high)
    across = flipped(low_link)
    outs = product(product(low_link, y), across)
    top = inverse((alpha[0] - outs[0], alpha[1] - outs[1]))
    states = [[read(own_ref, k, 2 * piece) for piece in range(3)] for k in range(2)]
    used = [chosen(high, state[1], state[2]) for state in states]
    weighted = product(rows(*used), y)
    moved = product(weighted, across)
    legs = [
        tuple(
            jnp.where(high, 0.0, s) + m[k * size : (k + 1) * size] for s, m in zip(states[k][1], moved)
        )
        for k in range(2)
    ]
    carried = product(rows(*legs), top)
    for k in range(2):
        part = slice(k * size, (k + 1) * size)
        own = product(
            cols((weighted[0][part], weighted[1][part]), (carried[0][part], carried[1][part])),
            rows(flipped(used[k]), flipped(legs[k])),
        )
        real_ref[k] = states[k][0][0] + own[0]
        imag_ref[k] = states[k][0][1] + own[1]

    def drain(level, stride):
        for copy in copies(level, stride):
            copy.wait_send()
        return 2 * stride

    lax.fori_loop(0, levels, drain, jnp.int32(1))


def shards(onsite_energy, onsite_mixing, hop_strength, hop_mixing, energy, broadening):
    size = onsite_mixing.shape[1]
    count = lax.axis_size("slab")
    levels = count.bit_length() - 1
    vmem = pl.BlockSpec(memory_space=pltpu.VMEM)
    smem = pl.BlockSpec(memory_space=pltpu.SMEM)
    out = jax.ShapeDtypeStruct(onsite_mixing.shape, jnp.float32)
    crit = pltpu.VMEM((levels, 2, size, size), jnp.float32)
    rest = pltpu.VMEM((levels, 4, size, size), jnp.float32)
    return pl.pallas_call(
        functools.partial(wire, count),
        out_shape=[out, out],
        in_specs=[smem] * 2 + [vmem] * 4,
        out_specs=[vmem, vmem],
        scratch_shapes=[crit, crit, rest, rest, pltpu.VMEM((2, 6, size, size), jnp.float32)]
        + [pltpu.SemaphoreType.DMA((levels,))] * 4,
        compiler_params=pltpu.CompilerParams(collective_id=0, has_side_effects=True),
        name="wire",
    )(energy, broadening, onsite_energy, onsite_mixing, hop_strength, hop_mixing)


def solution(mesh):
    return jax.shard_map(
        shards,
        mesh=mesh,
        in_specs=(
            P("slab", None),
            P("slab", None, None),
            P("slab", None),
            P("slab", None, None),
            P("energy"),
            P("energy"),
        ),
        out_specs=(P(("energy", "slab"), None, None), P(("energy", "slab"), None, None)),
        check_vma=False,
    )
```
